32 devices in a mesh: dp: 8 (over z, y), tp: 4 (over x, core).
Axes of the slice: x: 2, y: 2, z: 4, core: 2. Of those that a mesh axis runs over, the one named last changes fastest.
Arguments:
- tokens: bfloat16 [768, 2880], P('dp', 'tp'), may hold values from -100 to 100
- attn_gain: float32 [2880], replicated, may hold values from 0.1 to 1.9
- w_query: bfloat16 [2880, 2048], P(None, 'tp'), may hold values from -0.109375 to 0.109375
- w_keyvalue: bfloat16 [2880, 8, 128], P(None, 'tp'), may hold values from -0.109375 to 0.109375
- attn_sinks: float32 [32], P('tp'), may hold values from 2 to 6
- w_out: bfloat16 [2048, 2880], P('tp'), may hold values from -0.125 to 0.125
- window_cache: bfloat16 [768, 8, 128, 128], P('dp', 'tp'), may hold values from -1000 to 1000
- positions: int32 [768], P('dp'), may hold values from 0 to 511
- moe_gain: float32 [2880], replicated, may hold values from 0.1 to 1.9
- router: bfloat16 [2880, 8], P('tp'), may hold values from -0.109375 to 0.109375
- gate_up: bfloat16 [8, 2880, 2, 2880], P('dp', None, None, 'tp'), may hold values from -0.109375 to 0.109375
- w_down: bfloat16 [8, 2880, 2880], P('dp', None, 'tp'), may hold values from -0.109375 to 0.109375
- expert_ids: int32 [768, 4], P('dp'), may hold values from 0 to 7, all different within a row; in each aligned block of 96 rows (0 to 95, 96 to 191, ...) at most 96 rows name the same one
Outputs:
- layer_out: float32 [768, 2880], P('dp', 'tp')
The draws below stay inside these ranges and needn't reach their ends.
Inputs may be any that keep to these rules, and one draw needn't show every extreme that they name: `expert_ids`: each row names 4 different experts. Within the rows of one index of dp no expert is named by more than 96 rows, a bound that some of these blocks reach.
All inputs are finite; a program needn't handle non-finite values.
Results may differ from the reference program's by a relative error of at most 0.0066.
Values may be sent and summed in bfloat16 or wider, within the bound.
A program may use at most 128 MiB of HBM per device.

```python
import math
import jax
import jax.numpy as jnp
import numpy as np
from jax import lax

D = 2880
QH = 32
KVH = 8
HD = 64
WINDOW = 128
TOP = 4
FF = 2880
TOK_DEV = 96
EXPERTS = 8
TOKENS = 768
CAP = 96
N_DP = 8


def draw_tokens(key, part):
    base_key, col_key, row_key = jax.random.split(key, 3)
    places = jnp.arange(D, dtype=jnp.float32) / D
    col_scale = jnp.power(10.0, 0.5 * places + 0.5 * jax.random.uniform(col_key, (D,)))
    base = jnp.clip(jax.random.normal(base_key, (TOKENS, D)), -4.0, 4.0)
    row_scale = jnp.power(10.0, jax.random.uniform(row_key, (TOKENS, 1)))
    return (0.1 * base * row_scale * col_scale[None, :]).astype(jnp.bfloat16)


def draw_window_cache(key, part):
    normal_key = jax.random.fold_in(key, 0)
    entries = jnp.clip(jax.random.normal(normal_key, (TOKENS, KVH, WINDOW, 2 * HD)), -6.0, 6.0)
    return entries.astype(jnp.bfloat16)


def touch_ends(result, key, smallest, high):
    spot = [jax.random.randint(jax.random.fold_in(key, axis), (), 0, length) for axis, length in enumerate(result.shape)]
    main_axis = result.shape.index(max(result.shape))
    next_to = spot[:main_axis] + [(spot[main_axis] + 1) % result.shape[main_axis]] + spot[main_axis + 1:]
    return result.at[tuple(spot)].set(smallest).at[tuple(next_to)].set(high)


def block_levels(key, extent, shards, smallest, high):
    loudness, own = 1.0, jax.random.fold_in(key, 6)
    for dim, parts in shards:
        draws = jnp.exp(jax.random.uniform(jax.random.fold_in(own, dim), (parts,), jnp.float32, smallest / len(shards), high / len(shards)))
        loudness = loudness * jnp.repeat(draws, extent[dim] // parts).reshape([-1 if axis == dim else 1 for axis in range(len(extent))])
    return loudness


def routed_block(own_key, own, number, rows, number_of, top, reach, slope):
    ranking = jax.random.permutation(own_key, number_of)
    crowded, ordinary = load_shares(number_of, rows * top, reach, slope, True), load_shares(number_of, rows * top, reach, slope, False)
    places = jnp.arange(number_of)

    def named(sizes, turn):
        used = int((sizes > 0).sum())
        fixed = max(1, used // 4)
        moved = fixed + (places - fixed + turn * (used - fixed)) % max(1, number_of - fixed)
        return jnp.zeros((number_of,), jnp.int32).at[ranking[jnp.where(places < fixed, places, moved)]].set(jnp.asarray(sizes, jnp.int32))

    sizes = jnp.where(number % 4 == 0, named(crowded, number // 4), named(ordinary, number - number // 4 - 1))
    mixed = jax.random.permutation(jax.random.fold_in(own, 3), number_of)
    donor, sink = mixed[0:number_of // 2 * 2:2], mixed[1:number_of // 2 * 2:2]
    slack = jnp.minimum(sizes[donor] - 1, reach - sizes[sink]) // 2
    slack = jnp.where((donor == ranking[0]) | (sink == ranking[0]) | (sizes[sink] == 0), 0, jnp.maximum(slack, 0))
    moved = jax.random.randint(jax.random.fold_in(own, 4), (number_of // 2,), 0, 1 << 20) % (slack + 1)
    sizes = sizes.at[donor].add(-moved).at[sink].add(moved)
    items = jnp.searchsorted(jnp.cumsum(sizes), jnp.arange(rows * top), side="right").astype(jnp.int32)
    listing = items.reshape(top, rows).T
    listing = listing[jax.random.permutation(jax.random.fold_in(own, 1), rows)]
    turn = jax.random.randint(jax.random.fold_in(own, 2), (rows, 1), 0, top)
    return jnp.take_along_axis(listing, (jnp.arange(top)[None, :] + turn) % top, axis=1)


def load_shares(number_of, total, limit, lean, full):
    weights = [(1 << 20) // math.isqrt(rank ** lean) + 1 for rank in range(1, number_of + 1)]
    largest = limit if full else min(limit, max(-(-total // number_of), total * weights[0] // sum(weights)))
    least = 1 if total - largest >= number_of - 1 else 0
    counts, surplus = [largest] + [least] * (number_of - 1), total - largest - least * (number_of - 1)
    while surplus > 0:
        candidates = [i for i in range(1, number_of) if counts[i] < largest] or [i for i in range(1, number_of) if counts[i] < limit]
        mass, left = sum([weights[i] for i in candidates]), surplus
        for i in candidates:
            more = min(limit - counts[i], max(1, left * weights[i] // mass), surplus)
            counts[i] = counts[i] + more
            surplus = surplus - more
    return np.array(counts)


def gaussian(stream_key, shape, spread, most, cuts=(), kind=jnp.bfloat16):
    drawn = spread * jax.random.normal(stream_key, shape, jnp.float32)
    if cuts:
        drawn = drawn * block_levels(stream_key, shape, cuts, -0.22, 0.18)
    return jnp.clip(drawn, -most, most).astype(kind)


def setup_inputs(seed: int = 0) -> dict:
    splits = jax.random.split(jax.random.key(seed), 14)
    tokens = draw_tokens(jax.random.fold_in(splits[13], 71), 0)
    attn_gain = jnp.clip(1.0 + 0.18 * jax.random.normal(splits[1], (D,), jnp.float32), 0.1, 1.9)
    w_query = gaussian(splits[2], (D, QH * HD), D ** -0.5, 0.109375, ((1, 4),))
    w_keyvalue = gaussian(splits[3], (D, KVH, 2 * HD), D ** -0.5, 0.109375, ((1, 4),))
    attn_sinks = jnp.clip(2.0 + 4.0 * jax.random.uniform(splits[4], (QH,), jnp.float32) ** block_levels(splits[4], (QH,), ((0, 4),), -0.2, 0.2), 2.0, 6.0)
    w_out = gaussian(splits[5], (QH * HD, D), (QH * HD) ** -0.5, 0.125, ((0, 4),))
    window_cache = draw_window_cache(jax.random.fold_in(splits[13], 71), 0)
    positions = touch_ends(jax.random.randint(splits[7], (TOKENS,), 0, 4 * WINDOW), jax.random.fold_in(splits[7], 1), 0, (4 * WINDOW) - 1).astype(jnp.int32)
    moe_gain = jnp.clip(1.0 + 0.18 * jax.random.normal(splits[8], (D,), jnp.float32), 0.1, 1.9)
    router = gaussian(splits[9], (D, EXPERTS), D ** -0.5, 0.109375, ((0, 4),))
    gate_up = gaussian(splits[10], (EXPERTS, D, 2, FF), D ** -0.5, 0.109375, ((0, 8), (3, 4)))
    w_down = gaussian(splits[11], (EXPERTS, FF, D), FF ** -0.5, 0.109375, ((0, 8), (2, 4)))
    expert_ids_keys = jax.random.split(jax.random.fold_in(splits[12], 1), TOKENS // TOK_DEV)
    expert_ids_turns = jax.random.permutation(jax.random.fold_in(splits[12], 3), TOKENS // TOK_DEV)
    expert_ids = jax.vmap(lambda own, number: routed_block(jax.random.fold_in(splits[12], 2), own, number, TOK_DEV, EXPERTS, TOP, CAP, 2))(expert_ids_keys, expert_ids_turns).reshape((TOKENS, TOP))
    return {"tokens": tokens, "attn_gain": attn_gain, "w_query": w_query, "w_keyvalue": w_keyvalue, "attn_sinks": attn_sinks, "w_out": w_out, "window_cache": window_cache, "positions": positions, "moe_gain": moe_gain, "router": router, "gate_up": gate_up, "w_down": w_down, "expert_ids": expert_ids}


norm_eps = 1e-05
rope_base = 150000.0
glu_alpha = 1.702

def rope_tables(positions, head_size):
    half_size = head_size // 2
    exponent = jnp.arange(half_size, dtype=jnp.float32) * (2.0 / head_size)
    inverse = jnp.power(jnp.float32(rope_base), -exponent)
    angles = positions.astype(jnp.float32)[:, None] * inverse[None, :]
    return (jnp.cos(angles), jnp.sin(angles))

def rotate(values, cosine, sine_table):
    half_size = values.shape[-1] // 2
    first_half = values[..., :half_size]
    second_half = values[..., half_size:]
    return jnp.concatenate([first_half * cosine - second_half * sine_table, second_half * cosine + first_half * sine_table], axis=-1)

def reference(tokens, attn_gain, w_query, w_keyvalue, attn_sinks, w_out, window_cache, positions, moe_gain, router, gate_up, w_down, expert_ids):
    seq_count, full_width = tokens.shape
    head_size = w_keyvalue.shape[2] // 2
    kv_heads = w_keyvalue.shape[1]
    q_heads = w_query.shape[1] // head_size
    group_size = q_heads // kv_heads
    window = window_cache.shape[2]
    tok_wide = tokens.astype(jnp.float32)
    attn_mean = lax.optimization_barrier(jnp.mean(tok_wide * tok_wide, axis=1, keepdims=True))
    normed = (tok_wide * lax.rsqrt(attn_mean + norm_eps) * attn_gain[None, :]).astype(jnp.bfloat16)
    queries = jnp.dot(normed, w_query, preferred_element_type=jnp.float32).reshape(seq_count, q_heads, head_size)
    fresh_rows = jnp.dot(normed, w_keyvalue.reshape(full_width, kv_heads * 2 * head_size), preferred_element_type=jnp.float32)
    fresh_rows = fresh_rows.reshape(seq_count, kv_heads, 2 * head_size)
    cosine, sine_table = rope_tables(positions, head_size)
    rot_queries = rotate(queries, cosine[:, None, :], sine_table[:, None, :]).astype(jnp.bfloat16)
    new_key = rotate(fresh_rows[..., :head_size], cosine[:, None, :], sine_table[:, None, :])
    new_entry = jnp.concatenate([new_key, fresh_rows[..., head_size:]], axis=-1).astype(jnp.bfloat16)
    slot_ids = jnp.arange(window, dtype=jnp.int32)
    is_current = slot_ids[None, :] == (positions % window)[:, None]
    cache_now = jnp.where(is_current[:, None, :, None], new_entry[:, :, None, :], window_cache)
    is_valid = (positions[:, None] - slot_ids[None, :]) % window <= positions[:, None]
    score_scale = head_size ** (-0.5)

    def attend_head(inputs):
        head_cache, head_query, head_sinks = inputs
        key_part = head_cache[..., :head_size].astype(jnp.float32)
        value_part = head_cache[..., head_size:].astype(jnp.float32)
        scores = jnp.einsum('sgh,swh->sgw', head_query.astype(jnp.float32), key_part) * score_scale
        scores = jnp.where(is_valid[:, None, :], scores, -jnp.inf)
        sink_col = head_sinks[None, :, None]
        peak_score = jnp.maximum(lax.optimization_barrier(jnp.max(scores, axis=-1, keepdims=True)), sink_col)
        raised = jnp.exp(scores - peak_score)
        denominator = lax.optimization_barrier(jnp.sum(raised, axis=-1, keepdims=True)) + jnp.exp(sink_col - peak_score)
        prob_bf = (raised / denominator).astype(jnp.bfloat16)
        return jnp.einsum('sgw,swh->sgh', prob_bf.astype(jnp.float32), value_part).astype(jnp.bfloat16)
    grouped = rot_queries.reshape(seq_count, kv_heads, group_size, head_size)
    attended = lax.map(attend_head, (jnp.transpose(cache_now, (1, 0, 2, 3)), jnp.transpose(grouped, (1, 0, 2, 3)), attn_sinks.reshape(kv_heads, group_size)))
    attended = jnp.transpose(attended, (1, 0, 2, 3)).reshape(seq_count, q_heads * head_size)
    residual = tok_wide + jnp.dot(attended, w_out, preferred_element_type=jnp.float32)
    moe_mean = lax.optimization_barrier(jnp.mean(residual * residual, axis=1, keepdims=True))
    scaled = residual * lax.rsqrt(moe_mean + norm_eps) * moe_gain[None, :]
    logits = jnp.dot(scaled, router.astype(jnp.float32), precision=lax.Precision.HIGHEST)
    hidden_rows = scaled.astype(jnp.bfloat16)
    experts = router.shape[1]
    expert_iota = jnp.arange(experts, dtype=jnp.int32)
    chosen = expert_ids[:, :, None] == expert_iota[None, None, :]
    picked = lax.optimization_barrier(jnp.sum(jnp.where(chosen, logits[:, None, :], 0.0), axis=-1))
    raised_logits = jnp.exp(picked)
    route_weights = raised_logits / lax.optimization_barrier(jnp.sum(raised_logits, axis=1, keepdims=True))
    per_group = seq_count // N_DP
    group_ids = expert_ids.reshape(N_DP, per_group * TOP)
    onehot = (group_ids[:, :, None] == expert_iota[None, None, :]).astype(jnp.int32)
    earlier = jnp.cumsum(onehot, axis=1) - onehot
    slot_of = lax.optimization_barrier(jnp.sum(earlier * onehot, axis=2))
    column = (jnp.arange(N_DP, dtype=jnp.int32)[:, None] * CAP + slot_of).reshape(-1).astype(jnp.int32)
    expert_flat = group_ids.reshape(-1).astype(jnp.int32)
    repeated = jnp.repeat(hidden_rows, TOP, axis=0)
    buffer_rows = jnp.zeros((experts, N_DP * CAP, full_width), jnp.bfloat16).at[expert_flat, column].set(repeated)
    ff_width = w_down.shape[1]

    def one_expert(inputs):
        block_rows, weights_in, weights_down = inputs
        mixed_in = jnp.dot(block_rows, weights_in.reshape(full_width, 2 * ff_width), preferred_element_type=jnp.float32)
        gate_part = mixed_in[:, :ff_width]
        up_part = mixed_in[:, ff_width:]
        act_rows = (gate_part * jax.nn.sigmoid(glu_alpha * gate_part) * (up_part + 1.0)).astype(jnp.bfloat16)
        return jnp.dot(act_rows, weights_down, preferred_element_type=jnp.float32).astype(jnp.bfloat16)
    outputs = lax.map(one_expert, (buffer_rows, gate_up, w_down))
    gathered = outputs[expert_flat, column].reshape(seq_count, TOP, full_width).astype(jnp.float32)
    combined = lax.optimization_barrier(jnp.sum(route_weights[:, :, None] * gathered, axis=1))
    return residual + combined
```

```python
import functools
import math

import jax
import jax.numpy as jnp
from jax import lax
from jax.experimental import pallas as pl
from jax.experimental.pallas import tpu as pltpu
from jax.sharding import PartitionSpec as P

norm_eps = 1e-05
rope_base = 150000.0
glu_alpha = 1.702


def rope_tables(positions, head_size):
    half_size = head_size // 2
    exponent = jnp.arange(half_size, dtype=jnp.float32) * (2.0 / head_size)
    inverse = jnp.power(jnp.float32(rope_base), -exponent)
    angles = positions.astype(jnp.float32)[:, None] * inverse[None, :]
    return (jnp.cos(angles), jnp.sin(angles))


def rotate(values, cosine, sine_table):
    half_size = values.shape[-1] // 2
    first_half = values[..., :half_size]
    second_half = values[..., half_size:]
    return jnp.concatenate(
        [
            first_half * cosine - second_half * sine_table,
            second_half * cosine + first_half * sine_table,
        ],
        axis=-1,
    )


MESH = pl.DeviceIdType.MESH
CORES = 2


def greet(partners):
    barrier = pltpu.get_barrier_semaphore()
    for partner in partners:
        pl.semaphore_signal(barrier, inc=1, device_id=partner, device_id_type=MESH)
    pl.semaphore_wait(barrier, len(partners))


def feature_gather_kernel(tp, chunks, x_ref, out_ref, buf, own_sem, send_x, send_c, recv):
    chips = tp // CORES
    dp_id = lax.axis_index("dp")
    me = lax.axis_index("tp")
    core = lax.rem(me, CORES)
    chip = me // CORES
    rows, cols = x_ref.shape
    step = rows // chunks
    twin = (dp_id, chip * CORES + (1 - core))
    others = [lax.rem(chip + d, chips) * CORES + core for d in range(1, chips)]
    sources = [lax.rem(chip + chips - d, chips) * CORES + core for d in range(1, chips)]
    own = pltpu.make_async_copy(x_ref, buf.at[me], own_sem)
    own.start()
    greet([twin] + [(dp_id, other) for other in others])

    def piece(k):
        return pl.ds(k * step, step)

    def send(src, origin, k, sem, target):
        return pltpu.make_async_remote_copy(
            src_ref=src, dst_ref=buf.at[origin, piece(k)], send_sem=sem,
            recv_sem=recv.at[origin, k], device_id=target, device_id_type=MESH)

    sent = []
    for k in range(chunks):
        for d in range(chips - 1):
            sent.append(send(x_ref.at[piece(k)], me, k, send_x.at[d, k], (dp_id, others[d])))
            sent[-1].start()
    for k in range(chunks):
        sent.append(send(x_ref.at[piece(k)], me, k, send_c.at[0, k], twin))
        sent[-1].start()
    own.wait()
    for k in range(chunks):
        for d in range(chips - 1):
            origin = sources[d]
            forward = send(buf.at[origin, piece(k)], origin, k, send_c.at[d + 1, k], twin)
            forward.wait_recv()
            forward.start()
            sent.append(forward)
        if k:
            finish(tp, k - 1, step, chip, core, chips, buf, recv, out_ref, send, twin)
    finish(tp, chunks - 1, step, chip, core, chips, buf, recv, out_ref, send, twin)
    for copy in sent:
        copy.wait_send()


def finish(tp, k, step, chip, core, chips, buf, recv, out_ref, send, twin):
    cols = buf.shape[2]
    part = pl.ds(k * step, step)
    for d in range(chips):
        origin = lax.rem(chip + d, chips) * CORES + (1 - core)
        pltpu.make_async_remote_copy(
            src_ref=buf.at[origin, part], dst_ref=buf.at[origin, part], send_sem=recv.at[origin, k],
            recv_sem=recv.at[origin, k], device_id=twin, device_id_type=MESH).wait_recv()
    for t in range(tp):
        out_ref[part, t * cols:(t + 1) * cols] = buf[t, part, :]


def feature_gather(x, tp, chunks, collective_id):
    rows, cols = x.shape
    chips = tp // CORES
    return pl.pallas_call(
        functools.partial(feature_gather_kernel, tp, chunks),
        out_shape=jax.ShapeDtypeStruct((rows, tp * cols), x.dtype),
        in_specs=[pl.BlockSpec(memory_space=pltpu.VMEM)],
        out_specs=pl.BlockSpec(memory_space=pltpu.VMEM),
        scratch_shapes=[
            pltpu.VMEM((tp, rows, cols), x.dtype),
            pltpu.SemaphoreType.DMA,
            pltpu.SemaphoreType.DMA((max(chips - 1, 1), chunks)),
            pltpu.SemaphoreType.DMA((chips, chunks)),
            pltpu.SemaphoreType.DMA((tp, chunks)),
        ],
        compiler_params=pltpu.CompilerParams(
            collective_id=collective_id, has_side_effects=True, vmem_limit_bytes=48 * 2**20),
        cost_estimate=pl.CostEstimate(flops=0, bytes_accessed=rows * cols * tp * 16, transcendentals=0),
    )(x)


def full_gather_kernel(dp, ny, tp, x_ref, out_ref, buf, own_sem, send_z, send_x, send_y, send_c, recv):
    nz, nx = dp // ny, tp // CORES
    dp_id = lax.axis_index("dp")
    me = lax.axis_index("tp")
    core, x = lax.rem(me, CORES), me // CORES
    z, y = dp_id // ny, lax.rem(dp_id, ny)
    rows, cols = x_ref.shape
    half = rows // 2

    def place(pz, py, px, pc=core):
        return (pz * ny + py, px * CORES + pc)

    def around(v, d, n):
        return lax.rem(v + d, n)

    own = pltpu.make_async_copy(x_ref, buf.at[dp_id, me], own_sem)
    own.start()
    twin = place(z, y, x, 1 - core)
    x_others = [place(z, y, around(x, d, nx)) for d in range(1, nx)]
    y_others = [place(z, around(y, d, ny), x) for d in range(1, ny)]
    ring = [place(lax.rem(z + d, nz), y, x) for d in sorted({1 % nz, nz - 1} - {0})]
    greet([twin] + x_others + y_others + ring)
    own.wait()

    def copy(origin, h, sem, target):
        view = buf.at[origin[0], origin[1], pl.ds(h * half, half)]
        return pltpu.make_async_remote_copy(
            src_ref=view, dst_ref=view, send_sem=sem.at[origin[0], origin[1] // CORES, h],
            recv_sem=recv.at[origin[0], origin[1], h], device_id=target, device_id_type=MESH)

    def arrived(origin, h):
        view = buf.at[origin[0], origin[1], pl.ds(h * half, half)]
        pltpu.make_async_remote_copy(
            src_ref=view, dst_ref=view, send_sem=recv.at[origin[0], origin[1], h],
            recv_sem=recv.at[origin[0], origin[1], h], device_id=twin, device_id_type=MESH).wait_recv()

    def to_x(origin, h, act):
        for d in range(nx - 1):
            act(copy(origin, h, send_x.at[d], x_others[d]))

    def to_y(origin, h, act):
        for d in range(ny - 1):
            act(copy(origin, h, send_y.at[d], y_others[d]))

    def to_twin(origin, h, act):
        act(copy(origin, h, send_c, twin))

    def start(c):
        c.start()

    def ended(c):
        c.wait_send()

    def spread(origin, act):
        to_x(origin, 0, act)
        to_y(origin, 1, act)
        to_y(origin, 0, act)
        to_x(origin, 1, act)
        for h in range(2):
            to_twin(origin, h, act)

    def sideways(pz, act, wait):
        for d in range(1, nx):
            origin = place(pz, y, around(x, d, nx))
            if wait:
                arrived(origin, 0)
            to_y(origin, 0, act)
            to_twin(origin, 0, act)
        for d in range(1, ny):
            origin = place(pz, around(y, d, ny), x)
            if wait:
                arrived(origin, 1)
            to_x(origin, 1, act)
            to_twin(origin, 1, act)

    def last(pz, act, wait):
        for d in range(1, ny):
            for e in range(nx):
                origin = place(pz, around(y, d, ny), around(x, e, nx))
                if wait:
                    arrived(origin, 0)
                to_twin(origin, 0, act)
        for d in range(1, nx):
            for e in range(ny):
                origin = place(pz, around(y, e, ny), around(x, d, nx))
                if wait:
                    arrived(origin, 1)
                to_twin(origin, 1, act)

    def above(pz, act):
        @pl.when(z > 0)
        def _():
            for h in range(2):
                act(copy(place(pz, y, x), h, send_z.at[0], place(z - 1, y, x)))

    def below(pz, act):
        @pl.when(z < nz - 1)
        def _():
            for h in range(2):
                act(copy(place(pz, y, x), h, send_z.at[1], place(z + 1, y, x)))

    mine = place(z, y, x)
    above(z, start)
    below(z, start)
    spread(mine, start)

    def first_wave(pz, onward):
        origin = place(pz, y, x)
        arrived(origin, 0)
        arrived(origin, 1)
        onward(pz, start)
        spread(origin, start)

    sideways(z, start, True)
    for s in range(1, nz):
        for pz, ok, onward in ((z - s, z - s >= 0, below), (z + s, z + s < nz, above)):
            pl.when(ok)(functools.partial(first_wave, pz, onward))
        for pz, ok in ((z - s, z - s >= 0), (z + s, z + s < nz)):
            pl.when(ok)(functools.partial(sideways, pz, start, True))
        if s == 1:
            last(z, start, True)
        else:
            for pz, ok in ((z - s + 1, z - s + 1 >= 0), (z + s - 1, z + s - 1 < nz)):
                pl.when(ok)(functools.partial(last, pz, start, True))
    for pz, ok in ((z - nz + 1, z - nz + 1 >= 0), (z + nz - 1, z + nz - 1 < nz)):
        pl.when(ok)(functools.partial(last, pz, start, True))

    for b in range(dp):
        for px in range(nx):
            for h in range(2):
                arrived((b, px * CORES + 1 - core), h)
        for t in range(tp):
            out_ref[b * rows:(b + 1) * rows, t * cols:(t + 1) * cols] = buf[b, t]

    def ends(pz, onward=None):
        if onward is not None:
            onward(pz, ended)
        spread(place(pz, y, x), ended)
        sideways(pz, ended, False)
        last(pz, ended, False)

    above(z, ended)
    below(z, ended)
    ends(z)
    for s in range(1, nz):
        for pz, ok, onward in ((z - s, z - s >= 0, below), (z + s, z + s < nz, above)):
            pl.when(ok)(functools.partial(ends, pz, onward))


def full_gather(x, dp, tp, collective_id):
    rows, cols = x.shape
    nx = tp // CORES
    ny = 2 ** (int(math.log2(dp)) // 2)
    per_piece = (dp, nx, 2)
    return pl.pallas_call(
        functools.partial(full_gather_kernel, dp, ny, tp),
        out_shape=jax.ShapeDtypeStruct((dp * rows, tp * cols), x.dtype),
        in_specs=[pl.BlockSpec(memory_space=pltpu.VMEM)],
        out_specs=pl.BlockSpec(memory_space=pltpu.VMEM),
        scratch_shapes=[
            pltpu.VMEM((dp, tp, rows, cols), x.dtype),
            pltpu.SemaphoreType.DMA,
            pltpu.SemaphoreType.DMA((2,) + per_piece),
            pltpu.SemaphoreType.DMA((max(nx - 1, 1),) + per_piece),
            pltpu.SemaphoreType.DMA((max(ny - 1, 1),) + per_piece),
            pltpu.SemaphoreType.DMA(per_piece),
            pltpu.SemaphoreType.DMA((dp, tp, 2)),
        ],
        compiler_params=pltpu.CompilerParams(
            collective_id=collective_id, has_side_effects=True, vmem_limit_bytes=48 * 2**20),
        cost_estimate=pl.CostEstimate(flops=0, bytes_accessed=rows * cols * dp * tp * 8, transcendentals=0),
    )(x)


def activate(mixed_in, ff_local):
    gate_part = mixed_in[..., :ff_local]
    up_part = mixed_in[..., ff_local:]
    return (gate_part * jax.nn.sigmoid(glu_alpha * gate_part) * (up_part + 1.0)).astype(
        jnp.bfloat16
    )


def on_device(
    tokens,
    attn_gain,
    w_query,
    w_keyvalue,
    attn_sinks,
    w_out,
    window_cache,
    positions,
    moe_gain,
    router,
    gate_up,
    w_down,
    expert_ids,
):
    tp_count = lax.axis_size("tp")
    dp_count = lax.axis_size("dp")
    seq_count, col_count = tokens.shape
    full_width = col_count * tp_count
    col_start = lax.axis_index("tp") * col_count
    head_size = w_keyvalue.shape[2] // 2
    kv_local = w_keyvalue.shape[1]
    q_local = w_query.shape[1] // head_size
    group_size = q_local // kv_local
    window = window_cache.shape[2]
    moe_slice = lax.dynamic_slice_in_dim(moe_gain, col_start, col_count)
    tok_wide = tokens.astype(jnp.float32)
    kv_flat = w_keyvalue.reshape(full_width, kv_local * 2 * head_size)
    whole_rows = feature_gather(tokens, tp_count, 2, 0).astype(jnp.float32)
    attn_sq = jnp.sum(whole_rows * whole_rows, axis=1, keepdims=True)
    piece_rows = (
        whole_rows * lax.rsqrt(attn_sq / full_width + norm_eps) * attn_gain[None, :]
    ).astype(jnp.bfloat16)
    queries = jnp.dot(piece_rows, w_query, preferred_element_type=jnp.float32)
    fresh_rows = jnp.dot(piece_rows, kv_flat, preferred_element_type=jnp.float32)
    cosine, sine_table = rope_tables(positions, head_size)
    rot_queries = rotate(
        queries.reshape(seq_count, q_local, head_size), cosine[:, None, :], sine_table[:, None, :]
    ).astype(jnp.bfloat16)
    fresh_rows = fresh_rows.reshape(seq_count, kv_local, 2 * head_size)
    new_key = rotate(fresh_rows[..., :head_size], cosine[:, None, :], sine_table[:, None, :])
    new_entry = jnp.concatenate([new_key, fresh_rows[..., head_size:]], axis=-1).astype(
        jnp.bfloat16
    )
    slot_ids = jnp.arange(window, dtype=jnp.int32)
    is_current = slot_ids[None, :] == (positions % window)[:, None]
    cache_now = jnp.where(is_current[:, None, :, None], new_entry[:, :, None, :], window_cache)
    is_valid = (positions[:, None] - slot_ids[None, :]) % window <= positions[:, None]
    grouped = rot_queries.reshape(seq_count, kv_local, group_size, head_size)
    scores = jnp.einsum(
        "skgh,skwh->skgw", grouped, cache_now[..., :head_size], preferred_element_type=jnp.float32
    ) * head_size ** (-0.5)
    scores = jnp.where(is_valid[:, None, None, :], scores, -jnp.inf)
    sink_col = attn_sinks.reshape(kv_local, group_size)[None, :, :, None]
    peak_score = jnp.maximum(jnp.max(scores, axis=-1, keepdims=True), sink_col)
    raised = jnp.exp(scores - peak_score)
    denominator = jnp.sum(raised, axis=-1, keepdims=True) + jnp.exp(sink_col - peak_score)
    prob_bf = (raised / denominator).astype(jnp.bfloat16)
    attended = jnp.einsum(
        "skgw,skwh->skgh", prob_bf, cache_now[..., head_size:], preferred_element_type=jnp.float32
    ).astype(jnp.bfloat16)
    partial_out = jnp.dot(
        attended.reshape(seq_count, q_local * head_size), w_out, preferred_element_type=jnp.float32
    )
    residual = tok_wide + lax.psum_scatter(
        partial_out.astype(jnp.bfloat16), "tp", scatter_dimension=1, tiled=True
    ).astype(jnp.float32)
    experts = router.shape[1]
    top_count = expert_ids.shape[1]
    local_experts = gate_up.shape[0]
    ff_local = gate_up.shape[3]
    capacity = min(seq_count, max(2, 8 * seq_count * top_count // (3 * experts)))
    moe_sq = jnp.sum(residual * residual, axis=1)
    router_wide = router.astype(jnp.float32)
    total_sq = lax.psum(moe_sq, "tp")
    moe_scale = lax.rsqrt(total_sq / full_width + norm_eps)[:, None]
    scaled = residual * moe_scale * moe_slice[None, :]
    logits = lax.psum(jnp.dot(scaled, router_wide, precision=lax.Precision.HIGHEST), "tp")
    hidden_rows = scaled.astype(jnp.bfloat16)
    expert_iota = jnp.arange(experts, dtype=jnp.int32)
    chosen = expert_ids[:, :, None] == expert_iota[None, None, :]
    picked = jnp.sum(jnp.where(chosen, logits[:, None, :], 0.0), axis=-1)
    raised_logits = jnp.exp(picked)
    route_weights = raised_logits / jnp.sum(raised_logits, axis=1, keepdims=True)
    gate_up_flat = gate_up.reshape(local_experts, full_width, 2 * ff_local)
    if capacity >= seq_count:
        token_weights = jnp.sum(jnp.where(chosen, route_weights[:, :, None], 0.0), axis=1)
        all_rows = full_gather(hidden_rows, dp_count, tp_count, 1)
        outs = []
        for e in range(local_experts):
            mixed_in = jnp.dot(all_rows, gate_up_flat[e], preferred_element_type=jnp.float32)
            act_rows = activate(mixed_in, ff_local)
            act_all = feature_gather(act_rows, tp_count, dp_count, 2 + e)
            outs.append(
                jnp.dot(act_all, w_down[e], preferred_element_type=jnp.float32).astype(jnp.bfloat16)
            )
        answered = jnp.stack(
            [out.reshape(dp_count, seq_count, col_count) for out in outs], axis=1
        )
        returned = lax.all_to_all(answered, "dp", split_axis=0, concat_axis=0, tiled=True)
        back = returned.reshape(experts, seq_count, col_count).astype(jnp.float32)
        total = residual
        for e in range(experts):
            total = total + token_weights[:, e : e + 1] * back[e]
        return total
    assign = expert_ids.reshape(-1)
    onehot = (assign[:, None] == expert_iota[None, :]).astype(jnp.int32)
    earlier = jnp.cumsum(onehot, axis=0) - onehot
    slot_of = jnp.sum(earlier * onehot, axis=1)
    target = (assign * capacity + slot_of).reshape(seq_count, top_count)
    spot_ids = jnp.arange(experts * capacity, dtype=jnp.int32)
    slot_hits = target[:, :, None] == spot_ids[None, None, :]
    placer = jnp.transpose(jnp.any(slot_hits, axis=1)).astype(jnp.bfloat16)
    combiner = jnp.sum(jnp.where(slot_hits, route_weights[:, :, None], 0.0), axis=1)
    placed = jnp.dot(placer, hidden_rows, preferred_element_type=jnp.float32).astype(jnp.bfloat16)
    mixed_in = jnp.einsum(
        "gecd,edf->gecf",
        lax.all_gather(
            lax.all_to_all(
                placed.reshape(dp_count, local_experts, capacity, hidden_rows.shape[1]),
                "dp",
                split_axis=0,
                concat_axis=0,
                tiled=True,
            ),
            "tp",
            axis=3,
            tiled=True,
        ),
        gate_up_flat,
        preferred_element_type=jnp.float32,
    )
    act_rows = activate(mixed_in, ff_local)
    answered = jnp.einsum(
        "gecf,efd->gecd",
        lax.all_gather(act_rows, "tp", axis=3, tiled=True),
        w_down,
        preferred_element_type=jnp.float32,
    ).astype(jnp.bfloat16)
    returned = lax.all_to_all(answered, "dp", split_axis=0, concat_axis=0, tiled=True)
    flat_back = returned.reshape(experts * capacity, col_count).astype(jnp.float32)
    moe_out = jnp.dot(combiner, flat_back, precision=lax.Precision.HIGHEST)
    return residual + moe_out


def solution(mesh):
    in_specs = (
        P("dp", "tp"),
        P(),
        P(None, "tp"),
        P(None, "tp", None),
        P("tp"),
        P("tp", None),
        P("dp", "tp", None, None),
        P("dp"),
        P(),
        P("tp", None),
        P("dp", None, None, "tp"),
        P("dp", None, "tp"),
        P("dp", None),
    )
    out_specs = P("dp", "tp")
    return jax.shard_map(
        on_device, mesh=mesh, in_specs=in_specs, out_specs=out_specs, check_vma=False
    )
```

```python
import functools
import math

import jax
import jax.numpy as jnp
from jax import lax
from jax.experimental import pallas as pl
from jax.experimental.pallas import tpu as pltpu
from jax.sharding import PartitionSpec as P

norm_eps = 1e-05
rope_base = 150000.0
glu_alpha = 1.702


def rope_tables(positions, head_size):
    half_size = head_size // 2
    exponent = jnp.arange(half_size, dtype=jnp.float32) * (2.0 / head_size)
    inverse = jnp.power(jnp.float32(rope_base), -exponent)
    angles = positions.astype(jnp.float32)[:, None] * inverse[None, :]
    return (jnp.cos(angles), jnp.sin(angles))


def rotate(values, cosine, sine_table):
    half_size = values.shape[-1] // 2
    first_half = values[..., :half_size]
    second_half = values[..., half_size:]
    return jnp.concatenate(
        [
            first_half * cosine - second_half * sine_table,
            second_half * cosine + first_half * sine_table,
        ],
        axis=-1,
    )


MESH = pl.DeviceIdType.MESH
CORES = 2


def greet(partners):
    barrier = pltpu.get_barrier_semaphore()
    for partner in partners:
        pl.semaphore_signal(barrier, inc=1, device_id=partner, device_id_type=MESH)
    pl.semaphore_wait(barrier, len(partners))


def feature_gather_kernel(tp, chunks, x_ref, out_ref, buf, own_sem, send_x, send_c, recv):
    chips = tp // CORES
    dp_id = lax.axis_index("dp")
    me = lax.axis_index("tp")
    core = lax.rem(me, CORES)
    chip = me // CORES
    rows, cols = x_ref.shape
    step = rows // chunks
    twin = (dp_id, chip * CORES + (1 - core))
    others = [lax.rem(chip + d, chips) * CORES + core for d in range(1, chips)]
    sources = [lax.rem(chip + chips - d, chips) * CORES + core for d in range(1, chips)]
    own = pltpu.make_async_copy(x_ref, buf.at[me], own_sem)
    own.start()
    greet([twin] + [(dp_id, other) for other in others])

    def piece(k):
        return pl.ds(k * step, step)

    def send(src, origin, k, sem, target):
        return pltpu.make_async_remote_copy(
            src_ref=src, dst_ref=buf.at[origin, piece(k)], send_sem=sem,
            recv_sem=recv.at[origin, k], device_id=target, device_id_type=MESH)

    sent = []
    for k in range(chunks):
        for d in range(chips - 1):
            sent.append(send(x_ref.at[piece(k)], me, k, send_x.at[d, k], (dp_id, others[d])))
            sent[-1].start()
    for k in range(chunks):
        sent.append(send(x_ref.at[piece(k)], me, k, send_c.at[0, k], twin))
        sent[-1].start()
    own.wait()
    for k in range(chunks):
        for d in range(chips - 1):
            origin = sources[d]
            forward = send(buf.at[origin, piece(k)], origin, k, send_c.at[d + 1, k], twin)
            forward.wait_recv()
            forward.start()
            sent.append(forward)
        if k:
            finish(tp, k - 1, step, chip, core, chips, buf, recv, out_ref, send, twin)
    finish(tp, chunks - 1, step, chip, core, chips, buf, recv, out_ref, send, twin)
    for copy in sent:
        copy.wait_send()


def finish(tp, k, step, chip, core, chips, buf, recv, out_ref, send, twin):
    cols = buf.shape[2]
    part = pl.ds(k * step, step)
    for d in range(chips):
        origin = lax.rem(chip + d, chips) * CORES + (1 - core)
        pltpu.make_async_remote_copy(
            src_ref=buf.at[origin, part], dst_ref=buf.at[origin, part], send_sem=recv.at[origin, k],
            recv_sem=recv.at[origin, k], device_id=twin, device_id_type=MESH).wait_recv()
    for t in range(tp):
        out_ref[part, t * cols:(t + 1) * cols] = buf[t, part, :]


def feature_gather(x, tp, chunks, collective_id):
    rows, cols = x.shape
    chips = tp // CORES
    return pl.pallas_call(
        functools.partial(feature_gather_kernel, tp, chunks),
        out_shape=jax.ShapeDtypeStruct((rows, tp * cols), x.dtype),
        in_specs=[pl.BlockSpec(memory_space=pltpu.VMEM)],
        out_specs=pl.BlockSpec(memory_space=pltpu.VMEM),
        scratch_shapes=[
            pltpu.VMEM((tp, rows, cols), x.dtype),
            pltpu.SemaphoreType.DMA,
            pltpu.SemaphoreType.DMA((max(chips - 1, 1), chunks)),
            pltpu.SemaphoreType.DMA((chips, chunks)),
            pltpu.SemaphoreType.DMA((tp, chunks)),
        ],
        compiler_params=pltpu.CompilerParams(
            collective_id=collective_id, has_side_effects=True, vmem_limit_bytes=48 * 2**20),
        cost_estimate=pl.CostEstimate(flops=0, bytes_accessed=rows * cols * tp * 16, transcendentals=0),
    )(x)


def share_sum_kernel(tp, scatter, x_ref, out_ref, buf, send_sem, recv_sem):
    chips = tp // CORES
    dp_id = lax.axis_index("dp")
    me = lax.axis_index("tp")
    core = lax.rem(me, CORES)
    chip = me // CORES
    others = [
        lax.rem(chip + d, chips) * CORES + c for d in range(1, chips) for c in range(CORES)
    ] + [chip * CORES + (1 - core)]
    greet([(dp_id, other) for other in others])
    sent = []
    for i, other in enumerate(others):
        sent.append(pltpu.make_async_remote_copy(
            src_ref=x_ref.at[other if scatter else 0], dst_ref=buf.at[me], send_sem=send_sem.at[i],
            recv_sem=recv_sem.at[me], device_id=(dp_id, other), device_id_type=MESH))
        sent[-1].start()
    total = x_ref[me if scatter else 0].astype(jnp.float32)
    for i in reversed(range(len(others))):
        other = others[i]
        pltpu.make_async_remote_copy(
            src_ref=buf.at[other], dst_ref=buf.at[other], send_sem=send_sem.at[i],
            recv_sem=recv_sem.at[other], device_id=(dp_id, other), device_id_type=MESH).wait_recv()
        total = total + buf[other].astype(jnp.float32)
    out_ref[...] = total
    for copy in sent:
        copy.wait_send()


def share_sum(x, tp, scatter, collective_id):
    rows, cols = x.shape[1:]
    return pl.pallas_call(
        functools.partial(share_sum_kernel, tp, scatter),
        out_shape=jax.ShapeDtypeStruct((rows, cols), jnp.float32),
        in_specs=[pl.BlockSpec(memory_space=pltpu.VMEM)],
        out_specs=pl.BlockSpec(memory_space=pltpu.VMEM),
        scratch_shapes=[
            pltpu.VMEM((tp, rows, cols), x.dtype),
            pltpu.SemaphoreType.DMA((tp - 1,)),
            pltpu.SemaphoreType.DMA((tp,)),
        ],
        compiler_params=pltpu.CompilerParams(
            collective_id=collective_id, has_side_effects=True, vmem_limit_bytes=16 * 2**20),
        cost_estimate=pl.CostEstimate(flops=0, bytes_accessed=rows * cols * tp * 16, transcendentals=0),
    )(x)


def full_gather_kernel(dp, ny, tp, x_ref, out_ref, buf, own_sem, send_z, send_x, send_y, send_c, recv):
    nz, nx = dp // ny, tp // CORES
    dp_id = lax.axis_index("dp")
    me = lax.axis_index("tp")
    core, x = lax.rem(me, CORES), me // CORES
    z, y = dp_id // ny, lax.rem(dp_id, ny)
    rows, cols = x_ref.shape
    half = rows // 2

    def place(pz, py, px, pc=core):
        return (pz * ny + py, px * CORES + pc)

    def around(v, d, n):
        return lax.rem(v + d, n)

    own = pltpu.make_async_copy(x_ref, buf.at[dp_id, me], own_sem)
    own.start()
    twin = place(z, y, x, 1 - core)
    x_others = [place(z, y, around(x, d, nx)) for d in range(1, nx)]
    y_others = [place(z, around(y, d, ny), x) for d in range(1, ny)]
    ring = [place(lax.rem(z + d, nz), y, x) for d in sorted({1 % nz, nz - 1} - {0})]
    greet([twin] + x_others + y_others + ring)
    own.wait()

    def copy(origin, h, sem, target):
        view = buf.at[origin[0], origin[1], pl.ds(h * half, half)]
        return pltpu.make_async_remote_copy(
            src_ref=view, dst_ref=view, send_sem=sem.at[origin[0], origin[1] // CORES, h],
            recv_sem=recv.at[origin[0], origin[1], h], device_id=target, device_id_type=MESH)

    def arrived(origin, h):
        view = buf.at[origin[0], origin[1], pl.ds(h * half, half)]
        pltpu.make_async_remote_copy(
            src_ref=view, dst_ref=view, send_sem=recv.at[origin[0], origin[1], h],
            recv_sem=recv.at[origin[0], origin[1], h], device_id=twin, device_id_type=MESH).wait_recv()

    def to_x(origin, h, act):
        for d in range(nx - 1):
            act(copy(origin, h, send_x.at[d], x_others[d]))

    def to_y(origin, h, act):
        for d in range(ny - 1):
            act(copy(origin, h, send_y.at[d], y_others[d]))

    def to_twin(origin, h, act):
        act(copy(origin, h, send_c, twin))

    def start(c):
        c.start()

    def ended(c):
        c.wait_send()

    def spread(origin, act):
        to_x(origin, 0, act)
        to_y(origin, 1, act)
        to_y(origin, 0, act)
        to_x(origin, 1, act)
        for h in range(2):
            to_twin(origin, h, act)

    def sideways(pz, act, wait):
        for d in range(1, nx):
            origin = place(pz, y, around(x, d, nx))
            if wait:
                arrived(origin, 0)
            to_y(origin, 0, act)
            to_twin(origin, 0, act)
        for d in range(1, ny):
            origin = place(pz, around(y, d, ny), x)
            if wait:
                arrived(origin, 1)
            to_x(origin, 1, act)
            to_twin(origin, 1, act)

    def last(pz, act, wait):
        for d in range(1, ny):
            for e in range(nx):
                origin = place(pz, around(y, d, ny), around(x, e, nx))
                if wait:
                    arrived(origin, 0)
                to_twin(origin, 0, act)
        for d in range(1, nx):
            for e in range(ny):
                origin = place(pz, around(y, e, ny), around(x, d, nx))
                if wait:
                    arrived(origin, 1)
                to_twin(origin, 1, act)

    def above(pz, act):
        @pl.when(z > 0)
        def _():
            for h in range(2):
                act(copy(place(pz, y, x), h, send_z.at[0], place(z - 1, y, x)))

    def below(pz, act):
        @pl.when(z < nz - 1)
        def _():
            for h in range(2):
                act(copy(place(pz, y, x), h, send_z.at[1], place(z + 1, y, x)))

    mine = place(z, y, x)
    above(z, start)
    below(z, start)
    spread(mine, start)

    def first_wave(pz, onward):
        origin = place(pz, y, x)
        arrived(origin, 0)
        arrived(origin, 1)
        onward(pz, start)
        spread(origin, start)

    sideways(z, start, True)
    for s in range(1, nz):
        for pz, ok, onward in ((z - s, z - s >= 0, below), (z + s, z + s < nz, above)):
            pl.when(ok)(functools.partial(first_wave, pz, onward))
        for pz, ok in ((z - s, z - s >= 0), (z + s, z + s < nz)):
            pl.when(ok)(functools.partial(sideways, pz, start, True))
        if s == 1:
            last(z, start, True)
        else:
            for pz, ok in ((z - s + 1, z - s + 1 >= 0), (z + s - 1, z + s - 1 < nz)):
                pl.when(ok)(functools.partial(last, pz, start, True))
    for pz, ok in ((z - nz + 1, z - nz + 1 >= 0), (z + nz - 1, z + nz - 1 < nz)):
        pl.when(ok)(functools.partial(last, pz, start, True))

    for b in range(dp):
        for px in range(nx):
            for h in range(2):
                arrived((b, px * CORES + 1 - core), h)
        for h in range(2):
            start_row = (h * dp + b) * half
            for t in range(tp):
                out_ref[start_row:start_row + half, t * cols:(t + 1) * cols] = buf[
                    b, t, h * half:(h + 1) * half
                ]

    def ends(pz, onward=None):
        if onward is not None:
            onward(pz, ended)
        spread(place(pz, y, x), ended)
        sideways(pz, ended, False)
        last(pz, ended, False)

    above(z, ended)
    below(z, ended)
    ends(z)
    for s in range(1, nz):
        for pz, ok, onward in ((z - s, z - s >= 0, below), (z + s, z + s < nz, above)):
            pl.when(ok)(functools.partial(ends, pz, onward))


def full_gather(x, dp, tp, collective_id):
    rows, cols = x.shape
    nx = tp // CORES
    ny = 2 ** (int(math.log2(dp)) // 2)
    per_piece = (dp, nx, 2)
    return pl.pallas_call(
        functools.partial(full_gather_kernel, dp, ny, tp),
        out_shape=jax.ShapeDtypeStruct((dp * rows, tp * cols), x.dtype),
        in_specs=[pl.BlockSpec(memory_space=pltpu.VMEM)],
        out_specs=pl.BlockSpec(memory_space=pltpu.VMEM),
        scratch_shapes=[
            pltpu.VMEM((dp, tp, rows, cols), x.dtype),
            pltpu.SemaphoreType.DMA,
            pltpu.SemaphoreType.DMA((2,) + per_piece),
            pltpu.SemaphoreType.DMA((max(nx - 1, 1),) + per_piece),
            pltpu.SemaphoreType.DMA((max(ny - 1, 1),) + per_piece),
            pltpu.SemaphoreType.DMA(per_piece),
            pltpu.SemaphoreType.DMA((dp, tp, 2)),
        ],
        compiler_params=pltpu.CompilerParams(
            collective_id=collective_id, has_side_effects=True, vmem_limit_bytes=48 * 2**20),
        cost_estimate=pl.CostEstimate(flops=0, bytes_accessed=rows * cols * dp * tp * 8, transcendentals=0),
    )(x)


def activate(mixed_in, ff_local):
    gate_part = mixed_in[..., :ff_local]
    up_part = mixed_in[..., ff_local:]
    return (gate_part * jax.nn.sigmoid(glu_alpha * gate_part) * (up_part + 1.0)).astype(
        jnp.bfloat16
    )


def on_device(
    tokens,
    attn_gain,
    w_query,
    w_keyvalue,
    attn_sinks,
    w_out,
    window_cache,
    positions,
    moe_gain,
    router,
    gate_up,
    w_down,
    expert_ids,
):
    tp_count = lax.axis_size("tp")
    dp_count = lax.axis_size("dp")
    seq_count, col_count = tokens.shape
    full_width = col_count * tp_count
    col_start = lax.axis_index("tp") * col_count
    head_size = w_keyvalue.shape[2] // 2
    kv_local = w_keyvalue.shape[1]
    q_local = w_query.shape[1] // head_size
    group_size = q_local // kv_local
    window = window_cache.shape[2]
    moe_slice = lax.dynamic_slice_in_dim(moe_gain, col_start, col_count)
    tok_wide = tokens.astype(jnp.float32)
    kv_flat = w_keyvalue.reshape(full_width, kv_local * 2 * head_size)
    whole_rows = feature_gather(tokens, tp_count, 2, 0).astype(jnp.float32)
    attn_sq = jnp.sum(whole_rows * whole_rows, axis=1, keepdims=True)
    piece_rows = (
        whole_rows * lax.rsqrt(attn_sq / full_width + norm_eps) * attn_gain[None, :]
    ).astype(jnp.bfloat16)
    queries = jnp.dot(piece_rows, w_query, preferred_element_type=jnp.float32)
    fresh_rows = jnp.dot(piece_rows, kv_flat, preferred_element_type=jnp.float32)
    cosine, sine_table = rope_tables(positions, head_size)
    rot_queries = rotate(
        queries.reshape(seq_count, q_local, head_size), cosine[:, None, :], sine_table[:, None, :]
    ).astype(jnp.bfloat16)
    fresh_rows = fresh_rows.reshape(seq_count, kv_local, 2 * head_size)
    new_key = rotate(fresh_rows[..., :head_size], cosine[:, None, :], sine_table[:, None, :])
    new_entry = jnp.concatenate([new_key, fresh_rows[..., head_size:]], axis=-1).astype(
        jnp.bfloat16
    )
    slot_ids = jnp.arange(window, dtype=jnp.int32)
    is_current = slot_ids[None, :] == (positions % window)[:, None]
    is_valid = (positions[:, None] - slot_ids[None, :]) % window <= positions[:, None]
    is_valid = is_valid & ~is_current
    grouped = rot_queries.reshape(seq_count, kv_local, group_size, head_size)
    scores = jnp.einsum(
        "skgh,skwh->skgw", grouped, window_cache[..., :head_size], preferred_element_type=jnp.float32
    ) * head_size ** (-0.5)
    scores = jnp.where(is_valid[:, None, None, :], scores, -jnp.inf)
    new_wide = new_entry.astype(jnp.float32)[:, :, None, :]
    new_score = jnp.sum(
        grouped.astype(jnp.float32) * new_wide[..., :head_size], axis=-1, keepdims=True
    ) * head_size ** (-0.5)
    sink_col = attn_sinks.reshape(kv_local, group_size)[None, :, :, None]
    peak_score = jnp.maximum(
        jnp.maximum(jnp.max(scores, axis=-1, keepdims=True), new_score), sink_col
    )
    raised = jnp.exp(scores - peak_score)
    raised_new = jnp.exp(new_score - peak_score)
    denominator = (
        jnp.sum(raised, axis=-1, keepdims=True) + raised_new + jnp.exp(sink_col - peak_score)
    )
    prob_bf = (raised / denominator).astype(jnp.bfloat16)
    prob_new = (raised_new / denominator).astype(jnp.bfloat16).astype(jnp.float32)
    attended = jnp.einsum(
        "skgw,skwh->skgh", prob_bf, window_cache[..., head_size:], preferred_element_type=jnp.float32
    )
    attended = (attended + prob_new * new_wide[..., head_size:]).astype(jnp.bfloat16)
    partial_out = jnp.einsum(
        "sh,htc->tsc",
        attended.reshape(seq_count, q_local * head_size),
        w_out.reshape(q_local * head_size, tp_count, col_count),
        preferred_element_type=jnp.float32,
    ).astype(jnp.bfloat16)
    residual = tok_wide + share_sum(partial_out, tp_count, True, 2)
    experts = router.shape[1]
    top_count = expert_ids.shape[1]
    local_experts = gate_up.shape[0]
    ff_local = gate_up.shape[3]
    capacity = min(seq_count, max(2, 8 * seq_count * top_count // (3 * experts)))
    moe_sq = jnp.sum(residual * residual, axis=1)
    router_wide = router.astype(jnp.float32)
    gained = residual * moe_slice[None, :]
    raw_logits = jnp.dot(gained, router_wide, precision=lax.Precision.HIGHEST)
    stats = share_sum(
        jnp.concatenate([moe_sq[:, None], raw_logits], axis=1)[None], tp_count, False, 3
    )
    moe_scale = lax.rsqrt(stats[:, :1] / full_width + norm_eps)
    logits = stats[:, 1:] * moe_scale
    hidden_rows = (gained * moe_scale).astype(jnp.bfloat16)
    expert_iota = jnp.arange(experts, dtype=jnp.int32)
    chosen = expert_ids[:, :, None] == expert_iota[None, None, :]
    picked = jnp.sum(jnp.where(chosen, logits[:, None, :], 0.0), axis=-1)
    raised_logits = jnp.exp(picked)
    route_weights = raised_logits / jnp.sum(raised_logits, axis=1, keepdims=True)
    gate_up_flat = gate_up.reshape(local_experts, full_width, 2 * ff_local)
    if capacity >= seq_count:
        token_weights = jnp.sum(jnp.where(chosen, route_weights[:, :, None], 0.0), axis=1)
        all_rows = full_gather(hidden_rows, dp_count, tp_count, 1)
        half = seq_count // 2
        part = dp_count * half
        acts = [
            activate(
                jnp.dot(all_rows, gate_up_flat[e], preferred_element_type=jnp.float32), ff_local
            )
            for e in range(local_experts)
        ]
        pieces = []
        for h in range(2):
            outs = []
            for e in range(local_experts):
                act_all = feature_gather(
                    acts[e][h * part : (h + 1) * part], tp_count, dp_count // 2, 4 + 2 * e + h
                )
                out = jnp.dot(act_all, w_down[e], preferred_element_type=jnp.float32)
                outs.append(out.astype(jnp.bfloat16).reshape(dp_count, half, col_count))
            returned = lax.all_to_all(
                jnp.stack(outs, axis=1), "dp", split_axis=0, concat_axis=0, tiled=True
            )
            back = returned.reshape(experts, half, col_count)
            mine = slice(h * half, (h + 1) * half)
            total = residual[mine]
            for e in range(experts):
                total = total + token_weights[mine, e : e + 1] * back[e].astype(jnp.float32)
            pieces.append(total)
        total = jnp.concatenate(pieces, axis=0)
        return total
    assign = expert_ids.reshape(-1)
    onehot = (assign[:, None] == expert_iota[None, :]).astype(jnp.int32)
    earlier = jnp.cumsum(onehot, axis=0) - onehot
    slot_of = jnp.sum(earlier * onehot, axis=1)
    target = (assign * capacity + slot_of).reshape(seq_count, top_count)
    spot_ids = jnp.arange(experts * capacity, dtype=jnp.int32)
    slot_hits = target[:, :, None] == spot_ids[None, None, :]
    placer = jnp.transpose(jnp.any(slot_hits, axis=1)).astype(jnp.bfloat16)
    combiner = jnp.sum(jnp.where(slot_hits, route_weights[:, :, None], 0.0), axis=1)
    placed = jnp.dot(placer, hidden_rows, preferred_element_type=jnp.float32).astype(jnp.bfloat16)
    mixed_in = jnp.einsum(
        "gecd,edf->gecf",
        lax.all_gather(
            lax.all_to_all(
                placed.reshape(dp_count, local_experts, capacity, hidden_rows.shape[1]),
                "dp",
                split_axis=0,
                concat_axis=0,
                tiled=True,
            ),
            "tp",
            axis=3,
            tiled=True,
        ),
        gate_up_flat,
        preferred_element_type=jnp.float32,
    )
    act_rows = activate(mixed_in, ff_local)
    answered = jnp.einsum(
        "gecf,efd->gecd",
        lax.all_gather(act_rows, "tp", axis=3, tiled=True),
        w_down,
        preferred_element_type=jnp.float32,
    ).astype(jnp.bfloat16)
    returned = lax.all_to_all(answered, "dp", split_axis=0, concat_axis=0, tiled=True)
    flat_back = returned.reshape(experts * capacity, col_count).astype(jnp.float32)
    moe_out = jnp.dot(combiner, flat_back, precision=lax.Precision.HIGHEST)
    return residual + moe_out


def solution(mesh):
    in_specs = (
        P("dp", "tp"),
        P(),
        P(None, "tp"),
        P(None, "tp", None),
        P("tp"),
        P("tp", None),
        P("dp", "tp", None, None),
        P("dp"),
        P(),
        P("tp", None),
        P("dp", None, None, "tp"),
        P("dp", None, "tp"),
        P("dp", None),
    )
    out_specs = P("dp", "tp")
    return jax.shard_map(
        on_device, mesh=mesh, in_specs=in_specs, out_specs=out_specs, check_vma=False
    )
```
